32 devices in a mesh: seq: 4 (over x, core), fsdp: 8 (over z, y).
Axes of the slice: x: 2, y: 2, z: 4, core: 2. Of those that a mesh axis runs over, the one named last changes fastest.
Arguments:
- bytes_in: bfloat16 [4, 2048, 1280], P('seq', 'fsdp'), may hold values from -12 to 12, as said below
- doc_lengths: int32 [8], replicated, may hold values from 1 to 2048, 8192 in all
- patch_offsets: int32 [4, 512], P('seq', 'fsdp'), may hold values from 0 to 256, as said below
- patch_counts: int32 [4, 8], P('seq', 'fsdp'), may hold values from 32 to 64, as said below
- w_query: bfloat16 [1280, 1280], replicated, may hold values from -0.15625 to 0.15625
- w_key: bfloat16 [1280, 1280], replicated, may hold values from -0.15625 to 0.15625
- w_value: bfloat16 [1280, 1280], replicated, may hold values from -0.15625 to 0.15625
- w_proj: bfloat16 [1280, 4096], replicated, may hold values from -0.15625 to 0.15625
- norm_gain: float32 [4096], replicated, may hold values from 0.1 to 1.9
- gate_w: bfloat16 [4096, 7168], P('fsdp', 'seq'), may hold values from -0.09375 to 0.09375
- up_w: bfloat16 [4096, 7168], P('fsdp', 'seq'), may hold values from -0.09375 to 0.09375
- d_hidden: bfloat16 [4, 512, 7168], P(None, 'fsdp', 'seq'), may hold values from -6 to 6
Outputs:
- hidden: bfloat16 [4, 512, 7168], P(None, 'fsdp', 'seq')
- grad_gate: float32 [4096, 7168], P('fsdp', 'seq')
- grad_up: float32 [4096, 7168], P('fsdp', 'seq')
- d_patches: float32 [4, 512, 4096], P('seq', 'fsdp')
The draws below stay inside these ranges and needn't reach their ends.
Inputs may be any that keep to these rules, and one draw needn't show every extreme that they name: `bytes_in`: byte states of order one. `patch_offsets`: in each device block of 64 slots, slot 0 holds 0, the first c slots hold strictly rising offsets, c being the block's entry of patch_counts, and the other slots hold 256. `patch_counts`: patches of one device block; 64 is reached by some block in every draw.
All inputs are finite; a program needn't handle non-finite values.
Results may differ from the reference program's by a relative error of at most 0.022.
Values may be sent and summed in bfloat16 or wider, within the bound.
No kernel may reach another device: no remote copies, remote signals or barrier semaphores. Data moves between devices by JAX's collectives and lax.ppermute only.
A program may use at most 192 MiB of HBM per device.

```python
import math
import jax
import jax.numpy as jnp
import numpy as np
from jax import lax

DL = 1280
HEAD = 128
D = 4096
FF = 7168
WINDOW = 512
BYTES_DEV = 256
PATCH_DEV = 64
PATCH_ROW = 512
BYTES = 8192
DOCS = 8
N_SEQ = 4
N_FSDP = 8


def draw_bytes_in(key, part):
    full_shape = (N_SEQ, N_FSDP * BYTES_DEV, DL)
    noise_key = jax.random.fold_in(jax.random.fold_in(key, 11), 0)
    normal_part = jax.random.normal(noise_key, full_shape, jnp.float32)
    return jnp.clip(normal_part, -6.0, 6.0).astype(jnp.bfloat16)


def patch_layout(key):
    shards = N_SEQ * N_FSDP
    count_key, busy_key, score_key = jax.random.split(jax.random.fold_in(key, 7), 3)
    counts = jax.random.randint(count_key, (shards,), PATCH_DEV // 2, PATCH_DEV + 1)
    busiest = jax.random.randint(busy_key, (), 0, shards)
    counts = jnp.where(jnp.arange(shards) == busiest, PATCH_DEV, counts).astype(jnp.int32)
    scores = jax.random.randint(score_key, (shards, BYTES_DEV - 1), 0, 1 << 16) * BYTES_DEV + jnp.arange(BYTES_DEV - 1)[None, :]
    order_rank = jnp.argsort(jnp.argsort(scores, axis=1), axis=1)
    chosen = order_rank < (counts - 1)[:, None]
    starts_at = jnp.concatenate([jnp.ones((shards, 1), bool), chosen], axis=1)
    slot_index = jnp.cumsum(starts_at.astype(jnp.int32), axis=1) - 1
    target = jnp.where(starts_at, slot_index, PATCH_DEV)
    positions = jnp.broadcast_to(jnp.arange(BYTES_DEV, dtype=jnp.int32)[None, :], (shards, BYTES_DEV))
    shard_rows = jnp.broadcast_to(jnp.arange(shards)[:, None], (shards, BYTES_DEV))
    offsets = jnp.full((shards, PATCH_DEV), BYTES_DEV, jnp.int32).at[shard_rows, target].set(positions, mode='drop')
    return (offsets.reshape(N_SEQ, N_FSDP * PATCH_DEV), counts.reshape(N_SEQ, N_FSDP))


def draw_patch_offsets(key, part):
    return patch_layout(key)[0]


def draw_patch_counts(key, part):
    return patch_layout(key)[1]


def block_levels(key, extent, cuts, least, largest):
    factor_of, own = 1.0, jax.random.fold_in(key, 6)
    for position, parts in cuts:
        steps = jnp.exp(jax.random.uniform(jax.random.fold_in(own, position), (parts,), jnp.float32, least / len(cuts), largest / len(cuts)))
        factor_of = factor_of * jnp.repeat(steps, extent[position] // parts).reshape([-1 if axis == position else 1 for axis in range(len(extent))])
    return factor_of


def length_profile(amount, total, bound, slope):
    portions = [(1 << 20) // math.isqrt(rank ** slope) + 1 for rank in range(2, amount + 1)]
    surplus, given = total - bound - (amount - 1), [1] * (amount - 1)
    while surplus > 0:
        free = [i for i in range(amount - 1) if given[i] < bound]
        mass, budget = sum([portions[i] for i in free]), surplus
        for i in free:
            addition = min(bound - given[i], max(1, budget * portions[i] // mass), surplus)
            given[i] = given[i] + addition
            surplus = surplus - addition
    return np.array([bound] + given)


def uneven(own_key, amount, total, limit, slope):
    if amount == 2:
        one = jax.random.randint(own_key, (), max(1, total - limit), min(limit, total - 1) + 1)
        return jnp.stack([one, total - one])
    tallies = jnp.asarray(length_profile(amount, total, limit, slope), jnp.int32)
    couples = (amount - 1) // 2
    donor, receiver = tallies[1:1 + 2 * couples:2], tallies[2:2 + 2 * couples:2]
    margin = jnp.minimum(donor - 1, limit - receiver)
    passed = jax.random.randint(jax.random.fold_in(own_key, 1), (couples,), 0, 1 << 20) % (margin + 1)
    tallies = tallies.at[1:1 + 2 * couples:2].set(donor - passed).at[2:2 + 2 * couples:2].set(receiver + passed)
    return tallies[jax.random.permutation(jax.random.fold_in(own_key, 2), amount)]


def noise(own_key, shape, scale, limit, pieces=(), kind=jnp.bfloat16):
    entries = scale * jax.random.normal(own_key, shape, jnp.float32)
    if pieces:
        entries = entries * block_levels(own_key, shape, pieces, -0.22, 0.18)
    return jnp.clip(entries, -limit, limit).astype(kind)


def setup_inputs(seed: int = 0) -> dict:
    streams_of = jax.random.split(jax.random.key(seed), 13)
    bytes_in = draw_bytes_in(jax.random.fold_in(streams_of[12], 71), 0)
    doc_lengths = uneven(streams_of[1], DOCS, BYTES, 4 * WINDOW, 2).astype(jnp.int32)
    patch_offsets = draw_patch_offsets(jax.random.fold_in(streams_of[12], 71), 0)
    patch_counts = draw_patch_counts(jax.random.fold_in(streams_of[12], 71), 0)
    w_query = noise(streams_of[4], (DL, DL), DL ** -0.5, 0.15625)
    w_key = noise(streams_of[5], (DL, DL), DL ** -0.5, 0.15625)
    w_value = noise(streams_of[6], (DL, DL), DL ** -0.5, 0.15625)
    w_proj = noise(streams_of[7], (DL, D), DL ** -0.5, 0.15625)
    norm_gain = jnp.clip(1.0 + 0.18 * jax.random.normal(streams_of[8], (D,), jnp.float32), 0.1, 1.9)
    gate_w = noise(streams_of[9], (D, FF), D ** -0.5, 0.09375, ((0, 8), (1, 4)))
    up_w = noise(streams_of[10], (D, FF), D ** -0.5, 0.09375, ((0, 8), (1, 4)))
    d_hidden = noise(streams_of[11], (N_SEQ, PATCH_ROW, FF), 1.0, 6.0, ((1, 8), (2, 4)))
    return {"bytes_in": bytes_in, "doc_lengths": doc_lengths, "patch_offsets": patch_offsets, "patch_counts": patch_counts, "w_query": w_query, "w_key": w_key, "w_value": w_value, "w_proj": w_proj, "norm_gain": norm_gain, "gate_w": gate_w, "up_w": up_w, "d_hidden": d_hidden}


epsilon = 1e-05
masked_score = -1e+30

def doc_index(doc_lengths, positions):
    starts = jnp.cumsum(doc_lengths) - doc_lengths
    inside = (starts[None, :] <= positions[:, None]).astype(jnp.int32)
    return (lax.optimization_barrier(jnp.sum(inside, axis=1)) - 1).astype(jnp.int32)

def window_attention(queries, key_rows, values, query_pos, key_pos, query_doc, key_doc):
    row_count = queries.shape[0]
    head_count = queries.shape[1] // HEAD
    query_heads = queries.reshape(row_count, head_count, HEAD).astype(jnp.float32)
    key_heads = key_rows.reshape(-1, head_count, HEAD).astype(jnp.float32)
    value_heads = values.reshape(-1, head_count, HEAD).astype(jnp.float32)
    scores = jnp.einsum('qhd,khd->hqk', query_heads, key_heads) / math.sqrt(HEAD)
    allowed = (key_pos[None, :] <= query_pos[:, None]) & (query_pos[:, None] - key_pos[None, :] < WINDOW)
    allowed = allowed & (key_pos[None, :] >= 0) & (key_doc[None, :] == query_doc[:, None])
    scores = jnp.where(allowed[None], scores, masked_score)
    row_max = lax.optimization_barrier(jnp.max(scores, axis=-1, keepdims=True))
    weights = jnp.exp(scores - row_max)
    weights = (weights / lax.optimization_barrier(jnp.sum(weights, axis=-1, keepdims=True))).astype(jnp.bfloat16)
    mixed = jnp.einsum('hqk,khd->qhd', weights.astype(jnp.float32), value_heads)
    return mixed.reshape(row_count, head_count * HEAD)

def pool_patches(states, offsets, count):
    length = states.shape[0]
    slot_count = offsets.shape[0]
    head_count = states.shape[1] // HEAD
    slot_ids = jnp.arange(slot_count, dtype=jnp.int32)
    present = slot_ids < count
    following = jnp.concatenate([offsets[1:], jnp.full((1,), length, jnp.int32)])
    patch_ends = jnp.where(slot_ids == count - 1, length, following)
    byte_ids = jnp.arange(length, dtype=jnp.int32)
    member = present[:, None] & (offsets[:, None] <= byte_ids[None, :]) & (byte_ids[None, :] < patch_ends[:, None])
    patch_sizes = lax.optimization_barrier(jnp.sum(member.astype(jnp.float32), axis=1, keepdims=True))
    summed = jnp.dot(member.astype(jnp.bfloat16), states, preferred_element_type=jnp.float32)
    pooled = (summed / jnp.maximum(patch_sizes, 1.0)).astype(jnp.bfloat16)
    pooled_heads = pooled.reshape(slot_count, head_count, HEAD).astype(jnp.float32)
    state_heads = states.reshape(length, head_count, HEAD).astype(jnp.float32)
    scores = jnp.einsum('jhd,bhd->hjb', pooled_heads, state_heads) / math.sqrt(HEAD)
    scores = jnp.where(member[None], scores, masked_score)
    row_max = lax.optimization_barrier(jnp.max(scores, axis=-1, keepdims=True))
    weights = jnp.exp(scores - row_max)
    weights = (weights / lax.optimization_barrier(jnp.sum(weights, axis=-1, keepdims=True))).astype(jnp.bfloat16)
    context = jnp.einsum('hjb,bhd->jhd', weights.astype(jnp.float32), state_heads)
    context = context.reshape(slot_count, head_count * HEAD)
    return jnp.where(present[:, None], context, 0.0).astype(jnp.bfloat16)

def reference(bytes_in, doc_lengths, patch_offsets, patch_counts, w_query, w_key, w_value, w_proj, norm_gain, gate_w, up_w, d_hidden):
    shards = N_SEQ * N_FSDP
    total = shards * BYTES_DEV
    states = bytes_in.reshape(total, DL)
    queries = jnp.dot(states, w_query, preferred_element_type=jnp.float32).astype(jnp.bfloat16)
    key_rows = jnp.dot(states, w_key, preferred_element_type=jnp.float32).astype(jnp.bfloat16)
    values = jnp.dot(states, w_value, preferred_element_type=jnp.float32).astype(jnp.bfloat16)
    reach = (WINDOW - 2 + BYTES_DEV) // BYTES_DEV * BYTES_DEV
    positions = jnp.arange(total, dtype=jnp.int32)
    docs = doc_index(doc_lengths, positions)
    key_padded = jnp.concatenate([jnp.zeros((reach, DL), key_rows.dtype), key_rows])
    value_padded = jnp.concatenate([jnp.zeros((reach, DL), values.dtype), values])
    pos_padded = jnp.arange(total + reach, dtype=jnp.int32) - reach
    doc_padded = jnp.concatenate([jnp.full((reach,), -1, jnp.int32), docs])

    def attend(shard):
        row_start = (shard * BYTES_DEV).astype(jnp.int32)
        return window_attention(lax.dynamic_slice_in_dim(queries, row_start, BYTES_DEV), lax.dynamic_slice_in_dim(key_padded, row_start, reach + BYTES_DEV), lax.dynamic_slice_in_dim(value_padded, row_start, reach + BYTES_DEV), lax.dynamic_slice_in_dim(positions, row_start, BYTES_DEV), lax.dynamic_slice_in_dim(pos_padded, row_start, reach + BYTES_DEV), lax.dynamic_slice_in_dim(docs, row_start, BYTES_DEV), lax.dynamic_slice_in_dim(doc_padded, row_start, reach + BYTES_DEV))
    mixed = lax.map(attend, jnp.arange(shards, dtype=jnp.int32)).reshape(total, DL)
    hidden_bytes = (states.astype(jnp.float32) + mixed).astype(jnp.bfloat16)
    contexts = lax.map(lambda item: pool_patches(item[0], item[1], item[2]), (hidden_bytes.reshape(shards, BYTES_DEV, DL), patch_offsets.reshape(shards, PATCH_DEV), patch_counts.reshape(shards)))
    features = jnp.dot(contexts.reshape(shards * PATCH_DEV, DL), w_proj, preferred_element_type=jnp.float32).astype(jnp.bfloat16)
    patch_float = features.astype(jnp.float32)
    inverse = lax.rsqrt(lax.optimization_barrier(jnp.mean(patch_float * patch_float, axis=1, keepdims=True)) + epsilon)
    normed = (patch_float * inverse * norm_gain).astype(jnp.bfloat16)
    gate_pre = jnp.dot(normed, gate_w, preferred_element_type=jnp.float32)
    up_pre = jnp.dot(normed, up_w, preferred_element_type=jnp.float32)
    sigmoid_gate = jax.nn.sigmoid(gate_pre)
    hidden = (gate_pre * sigmoid_gate * up_pre).astype(jnp.bfloat16)
    cotangent = d_hidden.reshape(shards * PATCH_DEV, FF).astype(jnp.float32)
    gate_grad = (cotangent * up_pre * sigmoid_gate * (1.0 + gate_pre * (1.0 - sigmoid_gate))).astype(jnp.bfloat16)
    up_grad = (cotangent * gate_pre * sigmoid_gate).astype(jnp.bfloat16)
    both_grads = jnp.concatenate([gate_grad, up_grad], axis=1).reshape(N_SEQ, N_FSDP, PATCH_DEV, 2 * FF)
    normed_blocks = normed.reshape(N_SEQ, N_FSDP, PATCH_DEV, D)

    def add_partial(total_grad, block_index):
        rows_normed = lax.dynamic_index_in_dim(normed_blocks, block_index, 1, keepdims=False).reshape(N_SEQ * PATCH_DEV, D)
        rows_grad = lax.dynamic_index_in_dim(both_grads, block_index, 1, keepdims=False).reshape(N_SEQ * PATCH_DEV, 2 * FF)
        partial_value = lax.dot_general(rows_normed, rows_grad, (((0,), (0,)), ((), ())), preferred_element_type=jnp.float32)
        partial_value = lax.optimization_barrier(partial_value.astype(jnp.bfloat16)).astype(jnp.float32)
        return (total_grad + partial_value, None)
    weight_total, ignored = lax.scan(add_partial, jnp.zeros((D, 2 * FF), jnp.float32), jnp.arange(N_FSDP, dtype=jnp.int32))
    slice_width = FF // N_SEQ

    def add_input(total_grad, block_index):
        column_start = (block_index * slice_width).astype(jnp.int32)
        gate_part = lax.dynamic_slice_in_dim(gate_grad, column_start, slice_width, 1)
        up_part = lax.dynamic_slice_in_dim(up_grad, column_start, slice_width, 1)
        gate_cols = lax.dynamic_slice_in_dim(gate_w, column_start, slice_width, 1)
        up_cols = lax.dynamic_slice_in_dim(up_w, column_start, slice_width, 1)
        partial_value = lax.dot_general(gate_part, gate_cols, (((1,), (1,)), ((), ())), preferred_element_type=jnp.float32)
        partial_value = partial_value + lax.dot_general(up_part, up_cols, (((1,), (1,)), ((), ())), preferred_element_type=jnp.float32)
        partial_value = lax.optimization_barrier(partial_value.astype(jnp.bfloat16)).astype(jnp.float32)
        return (total_grad + partial_value, None)
    normed_grad, unused = lax.scan(add_input, jnp.zeros((shards * PATCH_DEV, D), jnp.float32), jnp.arange(N_SEQ, dtype=jnp.int32))
    scaled = norm_gain * normed_grad
    patch_grad = inverse * scaled - patch_float * (inverse * inverse * inverse) * lax.optimization_barrier(jnp.mean(scaled * patch_float, axis=1, keepdims=True))
    return (hidden.reshape(N_SEQ, N_FSDP * PATCH_DEV, FF), weight_total[:, :FF], weight_total[:, FF:], patch_grad.reshape(N_SEQ, N_FSDP * PATCH_DEV, D))
```

```python
import math

import jax
import jax.numpy as jnp
from jax import lax
from jax.sharding import Mesh
from jax.sharding import PartitionSpec as P

HEAD = 128
WINDOW = 512


epsilon = 1e-05
masked_score = -1e30


ROW_AXES = ("x", "core")
COL_AXES = ("a", "c", "b")
ALL_AXES = ROW_AXES + COL_AXES
CHUNK = 256


def shifted(shard, axis, by):
    devices = lax.axis_size(axis)
    pairs = [(i, i + by) for i in range(devices) if 0 <= i + by < devices]
    return lax.ppermute(shard, axis, pairs)


def turned(shard, axis, by):
    devices = lax.axis_size(axis)
    return lax.ppermute(shard, axis, [(i, (i + by) % devices) for i in range(devices)])


def pick(array, index, dim):
    return lax.dynamic_index_in_dim(array, index, dim, keepdims=False)


def put(buffer, block, index, dim):
    return lax.dynamic_update_slice_in_dim(buffer, jnp.expand_dims(block, dim), index, dim)


def collected(block, axis, dim):
    devices = lax.axis_size(axis)
    me = lax.axis_index(axis)
    shape = block.shape[:dim] + (devices,) + block.shape[dim:]
    result = put(jnp.zeros(shape, block.dtype), block, me, dim)
    for by in range(1, devices):
        result = put(result, turned(block, axis, by), (me - by) % devices, dim)
    return result


def summed_own(parts, axis, dim):
    devices = lax.axis_size(axis)
    me = lax.axis_index(axis)
    total = pick(parts, me, dim).astype(jnp.float32)
    for by in range(1, devices):
        sent = pick(parts, (me + by) % devices, dim).astype(jnp.bfloat16)
        total = total + turned(sent, axis, by).astype(jnp.float32)
    return total


def doc_index(doc_lengths, positions):
    starts = jnp.cumsum(doc_lengths) - doc_lengths
    inside = (starts[None, :] <= positions[:, None]).astype(jnp.int32)
    return jnp.sum(inside, axis=1) - 1


def window_attention(queries, key_rows, values, query_pos, key_pos, query_doc, key_doc):
    row_count = queries.shape[0]
    head_count = queries.shape[1] // HEAD
    query_heads = queries.reshape(row_count, head_count, HEAD)
    key_heads = key_rows.reshape(-1, head_count, HEAD)
    value_heads = values.reshape(-1, head_count, HEAD)
    scores = jnp.einsum(
        "qhd,khd->hqk", query_heads, key_heads, preferred_element_type=jnp.float32
    ) / math.sqrt(HEAD)
    allowed = (key_pos[None, :] <= query_pos[:, None]) & (
        query_pos[:, None] - key_pos[None, :] < WINDOW
    )
    allowed = allowed & (key_pos[None, :] >= 0) & (key_doc[None, :] == query_doc[:, None])
    scores = jnp.where(allowed[None], scores, masked_score)
    row_max = jnp.max(scores, axis=-1, keepdims=True)
    weights = jnp.exp(scores - row_max)
    weights = (weights / jnp.sum(weights, axis=-1, keepdims=True)).astype(jnp.bfloat16)
    mixed = jnp.einsum("hqk,khd->qhd", weights, value_heads, preferred_element_type=jnp.float32)
    return mixed.reshape(row_count, head_count * HEAD)


def pool_patches(states, offsets, count):
    length = states.shape[0]
    slot_count = offsets.shape[0]
    head_count = states.shape[1] // HEAD
    slot_ids = jnp.arange(slot_count, dtype=jnp.int32)
    present = slot_ids < count
    following = jnp.concatenate([offsets[1:], jnp.full((1,), length, jnp.int32)])
    patch_ends = jnp.where(slot_ids == count - 1, length, following)
    byte_ids = jnp.arange(length, dtype=jnp.int32)
    member = (
        present[:, None]
        & (offsets[:, None] <= byte_ids[None, :])
        & (byte_ids[None, :] < patch_ends[:, None])
    )
    patch_sizes = jnp.sum(member.astype(jnp.float32), axis=1, keepdims=True)
    summed = jnp.dot(member.astype(jnp.bfloat16), states, preferred_element_type=jnp.float32)
    pooled = (summed / jnp.maximum(patch_sizes, 1.0)).astype(jnp.bfloat16)
    pooled_heads = pooled.reshape(slot_count, head_count, HEAD)
    state_heads = states.reshape(length, head_count, HEAD)
    scores = jnp.einsum(
        "jhd,bhd->hjb", pooled_heads, state_heads, preferred_element_type=jnp.float32
    ) / math.sqrt(HEAD)
    scores = jnp.where(member[None], scores, masked_score)
    row_max = jnp.max(scores, axis=-1, keepdims=True)
    weights = jnp.exp(scores - row_max)
    weights = (weights / jnp.sum(weights, axis=-1, keepdims=True)).astype(jnp.bfloat16)
    context = jnp.einsum("hjb,bhd->jhd", weights, state_heads, preferred_element_type=jnp.float32)
    context = context.reshape(slot_count, head_count * HEAD)
    return jnp.where(present[:, None], context, 0.0).astype(jnp.bfloat16)


def shards(
    bytes_in,
    doc_lengths,
    patch_offsets,
    patch_counts,
    w_query,
    w_key,
    w_value,
    w_proj,
    norm_gain,
    gate_w,
    up_w,
    d_hidden,
):
    bf16, f32 = jnp.bfloat16, jnp.float32
    x_count, core_count = lax.axis_size("x"), lax.axis_size("core")
    a_count, c_count, b_count = (lax.axis_size(axis) for axis in COL_AXES)
    a_own, c_own, b_own = (lax.axis_index(axis) for axis in COL_AXES)
    states = bytes_in[0]
    length = states.shape[0]
    hop_count = (WINDOW - 2 + length) // length
    first_pos = lax.axis_index(ALL_AXES) * length

    state_parts = [states]
    for distance in range(1, hop_count + 1):
        state_parts.insert(0, shifted(states, ALL_AXES, distance))
    queries = jnp.dot(states, w_query, preferred_element_type=f32).astype(bf16)
    key_all = jnp.concatenate(
        [jnp.dot(part, w_key, preferred_element_type=f32).astype(bf16) for part in state_parts]
    )
    value_all = jnp.concatenate(
        [jnp.dot(part, w_value, preferred_element_type=f32).astype(bf16) for part in state_parts]
    )
    query_pos = first_pos + jnp.arange(length, dtype=jnp.int32)
    key_pos = first_pos - hop_count * length + jnp.arange((hop_count + 1) * length, dtype=jnp.int32)
    key_doc = doc_index(doc_lengths, key_pos)
    query_doc = key_doc[hop_count * length :]
    mixed = window_attention(queries, key_all, value_all, query_pos, key_pos, query_doc, key_doc)
    hidden_bytes = (states.astype(f32) + mixed).astype(bf16)
    context = pool_patches(hidden_bytes, patch_offsets[0], patch_counts[0, 0])
    slot_count = context.shape[0]

    rows, units = gate_w.shape
    sub = units // c_count
    spans = [(start, min(CHUNK, sub - start)) for start in range(0, sub, CHUNK)]
    gate_w, up_w, d_hidden, *_ = lax.optimization_barrier((gate_w, up_w, d_hidden, *state_parts[:-1]))
    cotangents = d_hidden.reshape(-1, units)
    cot_rows = cotangents.shape[0]
    cot_all = jnp.zeros((c_count, cot_rows, sub), bf16)
    for by in range(c_count):
        part = lax.dynamic_slice_in_dim(cotangents, (c_own + by) % c_count * sub, sub, 1)
        part = turned(part, "c", by) if by else part
        cot_all = put(cot_all, part, (c_own - by) % c_count, 0)
    cot_all = cot_all.reshape(c_count * cot_rows, sub)

    chunk_weights = []
    for start, width in spans:
        top = jnp.zeros((c_count, rows, 2 * width), bf16)
        for by in range(c_count):
            first = (c_own + by) % c_count * sub + start
            part = jnp.concatenate(
                [lax.dynamic_slice_in_dim(w, first, width, 1) for w in (gate_w, up_w)], axis=1
            )
            part = turned(part, "c", by) if by else part
            top = put(top, part, (c_own - by) % c_count, 0)
        top = top.reshape(c_count * rows, 2 * width)
        chunk_weights.append(
            jnp.concatenate([top] + [turned(top, "b", by) for by in range(1, b_count)])
        )

    features = jnp.dot(context, w_proj, preferred_element_type=f32).astype(bf16)
    own_float = features.astype(f32)
    model_width = own_float.shape[1]
    own_inverse = lax.rsqrt(jnp.mean(own_float * own_float, axis=1, keepdims=True) + epsilon)
    normed = (own_float * own_inverse * norm_gain).astype(bf16)
    blocks = normed.reshape(slot_count, a_count, c_count, b_count, rows)
    blocks = jnp.stack(
        [pick(blocks, (b_own - by) % b_count, 3) for by in range(b_count)], axis=2
    )
    part_width = model_width // a_count
    quarter = part_width // b_count
    blocks = blocks.reshape(slot_count, a_count, part_width)
    normed_parts = []
    for by in range(a_count):
        part = pick(blocks, (a_own - by) % a_count, 1)
        part = turned(part, "a", -by) if by else part
        part = collected(part, "core", 0)
        part = collected(part, "x", 0)
        part = collected(part, "c", 0)
        normed_parts.append(part.reshape(-1, part_width))
    normed_all = jnp.concatenate(normed_parts)

    hidden_parts = []
    weight_grads = []
    input_partial = None
    for (start, width), weight in zip(spans, chunk_weights):
        pre = None
        for by in range(1, a_count):
            sent = jnp.dot(normed_parts[by], weight, preferred_element_type=f32).astype(bf16)
            sent = turned(sent, "a", by).astype(f32)
            pre = sent if pre is None else pre + sent
        own = jnp.dot(normed_parts[0], weight, preferred_element_type=f32)
        pre = own if pre is None else own + pre
        gate_pre, up_pre = pre[:, :width], pre[:, width:]
        cotangent = cot_all[:, start : start + width].astype(f32)
        sigmoid_gate = jax.nn.sigmoid(gate_pre)
        hidden_parts.append((gate_pre * sigmoid_gate * up_pre).astype(bf16))
        gate_grad = cotangent * up_pre * sigmoid_gate * (1.0 + gate_pre * (1.0 - sigmoid_gate))
        up_grad = cotangent * gate_pre * sigmoid_gate
        grads = jnp.concatenate([gate_grad.astype(bf16), up_grad.astype(bf16)], axis=1)
        grads_all = jnp.concatenate(
            [grads] + [turned(grads, "a", -by) for by in range(1, a_count)]
        )

        total = None
        for by in [*range(1, b_count), 0]:
            partial = lax.dot_general(
                normed_all[:, by * quarter : (by + 1) * quarter],
                grads_all,
                (((0,), (0,)), ((), ())),
                preferred_element_type=f32,
            )
            if by:
                partial = turned(partial.astype(bf16), "b", -by).astype(f32)
            total = partial if total is None else total + partial
        total = total.reshape(c_count, rows, 2 * width)
        mine = [pick(total, c_own, 0)]
        for by in range(1, c_count):
            sent = pick(total, (c_own + by) % c_count, 0).astype(bf16)
            mine.append(turned(sent, "c", by).astype(f32))
        weight_grads.append(mine)

        partial = lax.dot_general(
            grads_all, weight, (((1,), (1,)), ((), ())), preferred_element_type=f32
        )
        input_partial = partial if input_partial is None else input_partial + partial

    hidden_own = jnp.concatenate(hidden_parts, axis=1).reshape(c_count, cot_rows, sub)
    hidden = jnp.zeros((cot_rows, c_count, sub), bf16)
    for by in range(c_count):
        part = pick(hidden_own, (c_own + by) % c_count, 0)
        part = turned(part, "c", by) if by else part
        hidden = put(hidden, part, (c_own - by) % c_count, 1)

    outs = []
    for side in range(2):
        out = jnp.zeros((rows, units), f32)
        for by in range(c_count):
            first = (c_own - by) % c_count * sub
            columns = jnp.concatenate(
                [
                    mine[by][:, side * width : (side + 1) * width]
                    for (start, width), mine in zip(spans, weight_grads)
                ],
                axis=1,
            )
            out = lax.dynamic_update_slice_in_dim(out, columns, first, 1)
        outs.append(out)

    partial = input_partial.reshape(
        a_count, c_count, x_count, core_count, slot_count, part_width
    )
    partial = summed_own(partial, "core", 3)
    partial = summed_own(partial, "x", 2)
    partial = summed_own(partial, "c", 1)
    normed_grad = jnp.zeros((slot_count, a_count, part_width), f32)
    for by in range(a_count):
        part = partial[by]
        part = turned(part.astype(bf16), "a", by).astype(f32) if by else part
        normed_grad = put(normed_grad, part, (a_own - by) % a_count, 1)
    normed_grad = normed_grad.reshape(slot_count, a_count, b_count, c_count, rows)
    ordered = jnp.zeros((slot_count, a_count, c_count, b_count, rows), f32)
    for by in range(b_count):
        ordered = put(ordered, normed_grad[:, :, by], (b_own - by) % b_count, 3)
    normed_grad = ordered.reshape(slot_count, model_width)
    scaled = norm_gain * normed_grad
    patch_grad = own_inverse * scaled - own_float * (
        own_inverse * own_inverse * own_inverse
    ) * jnp.mean(scaled * own_float, axis=1, keepdims=True)
    seq_count = d_hidden.shape[0]
    return (hidden.reshape(seq_count, slot_count, units), outs[0], outs[1], patch_grad[None])


def halved(count):
    return 2 if count % 2 == 0 else 1


def solution(mesh):
    seq_count, fsdp_count = mesh.shape["seq"], mesh.shape["fsdp"]
    core_count, b_count = halved(seq_count), halved(fsdp_count)
    c_count = halved(fsdp_count // b_count)
    fine = Mesh(
        mesh.devices.reshape(
            seq_count // core_count, core_count, fsdp_count // (b_count * c_count), c_count, b_count
        ),
        ALL_AXES,
    )
    return jax.shard_map(
        shards,
        mesh=fine,
        in_specs=(
            P(ROW_AXES, COL_AXES, None),
            P(),
            P(ROW_AXES, COL_AXES),
            P(ROW_AXES, COL_AXES),
            P(),
            P(),
            P(),
            P(),
            P(),
            P(COL_AXES, ROW_AXES),
            P(COL_AXES, ROW_AXES),
            P(None, COL_AXES, ROW_AXES),
        ),
        out_specs=(
            P(None, COL_AXES, ROW_AXES),
            P(COL_AXES, ROW_AXES),
            P(COL_AXES, ROW_AXES),
            P(ROW_AXES, COL_AXES, None),
        ),
        check_vma=False,
    )
```

```python
import math

import jax
import jax.numpy as jnp
from jax import lax
from jax.experimental import pallas as pl
from jax.experimental.pallas import tpu as pltpu
from jax.sharding import Mesh
from jax.sharding import PartitionSpec as P


HEAD = 128
WINDOW = 512


epsilon = 1e-05
masked_score = -1e30


ROW_AXES = ("x", "core")
COL_AXES = ("a", "c", "b")
ALL_AXES = ROW_AXES + COL_AXES
CHUNK = 256


def shifted(shard, axis, by):
    devices = lax.axis_size(axis)
    pairs = [(i, i + by) for i in range(devices) if 0 <= i + by < devices]
    return lax.ppermute(shard, axis, pairs)


def turned(shard, axis, by):
    devices = lax.axis_size(axis)
    if by % devices == 0:
        return shard
    return lax.ppermute(shard, axis, [(i, (i + by) % devices) for i in range(devices)])


def chosen(blocks, index):
    result = blocks[0]
    for k in range(1, len(blocks)):
        result = jnp.where(index == k, blocks[k], result)
    return result


def split(array, count, dim):
    return jnp.split(array, count, axis=dim) if count > 1 else [array]


def after(value, *others):
    return lax.optimization_barrier((value, *others))[0]


def own_sum(partial, axis, dim, order=None):
    devices = lax.axis_size(axis)
    blocks = split(partial, devices, dim)
    total = blocks[0].astype(jnp.float32)
    for k in range(1, devices):
        sent = blocks[k].astype(jnp.bfloat16)
        if order is not None:
            sent = order(sent, k)
        total = total + turned(sent, axis, -k).astype(jnp.float32)
    return total


def doc_index(doc_lengths, positions):
    starts = jnp.cumsum(doc_lengths) - doc_lengths
    inside = (starts[None, :] <= positions[:, None]).astype(jnp.int32)
    return jnp.sum(inside, axis=1) - 1


def cost(flops, arrays, transcendentals=0):
    moved = sum(a.size * a.dtype.itemsize for a in arrays)
    return pl.CostEstimate(flops=flops, bytes_accessed=moved, transcendentals=transcendentals)


def dot(lhs, rhs, lhs_dim=1, rhs_dim=0):
    return lax.dot_general(
        lhs, rhs, (((lhs_dim,), (rhs_dim,)), ((), ())), preferred_element_type=jnp.float32
    )


def softmax(scores):
    weights = jnp.exp(scores - jnp.max(scores, axis=-1, keepdims=True))
    return (weights / jnp.sum(weights, axis=-1, keepdims=True)).astype(jnp.bfloat16)


def byte_layer_kernel(
    q_ref, k_ref, v_ref, h_ref, qdoc_ref, kdoc_ref, start_ref, end_ref, present_ref, out_ref, bias_ref
):
    length, reach = q_ref.shape[0], k_ref.shape[0] - q_ref.shape[0]

    @pl.when(pl.program_id(0) == 0)
    def _():
        row = lax.broadcasted_iota(jnp.int32, bias_ref.shape, 0)
        back = row + reach - lax.broadcasted_iota(jnp.int32, bias_ref.shape, 1)
        allowed = (back >= 0) & (back < WINDOW) & (qdoc_ref[...] == kdoc_ref[...])
        bias_ref[...] = jnp.where(allowed, 0.0, masked_score)

    scores = dot(q_ref[...], k_ref[...], 1, 1) / math.sqrt(HEAD)
    weights = softmax(jnp.where(bias_ref[...] == 0.0, scores, masked_score))
    mixed = dot(weights, v_ref[...])
    states = (h_ref[...].astype(jnp.float32) + mixed).astype(jnp.bfloat16)
    present = present_ref[...] > 0
    ids = lax.broadcasted_iota(jnp.int32, (start_ref.shape[0], length), 1)
    member = present & (start_ref[...] <= ids) & (ids < end_ref[...])
    counts = jnp.where(member, 1.0, 0.0)
    sizes = jnp.sum(counts, axis=1, keepdims=True)
    pooled = (dot(counts.astype(jnp.bfloat16), states) / jnp.maximum(sizes, 1.0)).astype(jnp.bfloat16)
    scores = dot(pooled, states, 1, 1) / math.sqrt(HEAD)
    weights = softmax(jnp.where(member, scores, masked_score))
    out_ref[...] = jnp.where(present, dot(weights, states), 0.0).astype(jnp.bfloat16)


def byte_layer(queries, key_all, value_all, states, query_doc, key_doc, offsets, count):
    length, width = queries.shape
    reach = key_all.shape[0]
    slot_count = offsets.shape[0]
    slots = jnp.arange(slot_count, dtype=jnp.int32)
    following = jnp.concatenate([offsets[1:], jnp.full((1,), length, jnp.int32)])
    ends = jnp.where(slots == count - 1, length, following)
    present = (slots < count).astype(jnp.int32)

    def head(rows):
        return pl.BlockSpec((rows, HEAD), lambda i: (0, i))

    def whole(shape):
        return pl.BlockSpec(shape, lambda i: (0, 0))

    column = whole((slot_count, 1))
    return pl.pallas_call(
        byte_layer_kernel,
        grid=(width // HEAD,),
        in_specs=[
            head(length),
            head(reach),
            head(reach),
            head(length),
            whole((length, 1)),
            whole((1, reach)),
            column,
            column,
            column,
        ],
        out_specs=head(slot_count),
        out_shape=jax.ShapeDtypeStruct((slot_count, width), jnp.bfloat16),
        scratch_shapes=[pltpu.VMEM((length, reach), jnp.float32)],
        cost_estimate=cost(4 * length * reach * width, (queries, key_all, value_all, states)),
        name="byte_layer",
    )(
        queries,
        key_all,
        value_all,
        states,
        query_doc[:, None],
        key_doc[None, :],
        offsets[:, None],
        ends[:, None],
        present[:, None],
    )


def tile(count):
    return 256 if count % 256 == 0 else count


def product(lhs_ref, weight_refs):
    depth = weight_refs[0].shape[0]
    total = None
    for k, ref in enumerate(weight_refs):
        term = dot(lhs_ref[:, k * depth : (k + 1) * depth], ref[...])
        total = term if total is None else total + term
    return total


def weight_specs(pieces, low, wide):
    return [pl.BlockSpec((piece.shape[0], wide), lambda i: (0, low // wide)) for piece in pieces]


def partial_sums(lhs, pieces, low, wide):
    def kernel(lhs_ref, *refs):
        refs[-1][...] = product(lhs_ref, refs[:-1]).astype(jnp.bfloat16)

    rows, depth = lhs.shape
    step = tile(rows)
    out = jax.ShapeDtypeStruct((rows, wide), jnp.bfloat16)
    return pl.pallas_call(
        kernel,
        grid=(rows // step,),
        in_specs=[pl.BlockSpec((step, depth), lambda i: (i, 0))] + weight_specs(pieces, low, wide),
        out_specs=pl.BlockSpec((step, wide), lambda i: (i, 0)),
        out_shape=out,
        cost_estimate=cost(2 * rows * depth * wide, (lhs, out, out)),
        name="partial_sums",
    )(lhs, *pieces)


def gates(lhs, pieces, low, wide, received, cotangents, start):
    width = wide // 2

    def kernel(lhs_ref, *refs):
        refs, (cot_ref, hidden_ref, grad_ref) = refs[:-3], refs[-3:]
        pre = product(lhs_ref, refs[: len(pieces)])
        for ref in refs[len(pieces) :]:
            pre = pre + ref[...].astype(jnp.float32)
        gate_pre, up_pre = pre[:, :width], pre[:, width:]
        cotangent = cot_ref[...].astype(jnp.float32)
        sigmoid_gate = jax.nn.sigmoid(gate_pre)
        hidden_ref[...] = (gate_pre * sigmoid_gate * up_pre).astype(jnp.bfloat16)
        gate_grad = cotangent * up_pre * sigmoid_gate * (1.0 + gate_pre * (1.0 - sigmoid_gate))
        grad_ref[:, :width] = gate_grad.astype(jnp.bfloat16)
        grad_ref[:, width:] = (cotangent * gate_pre * sigmoid_gate).astype(jnp.bfloat16)

    rows, depth = lhs.shape
    step = tile(rows)
    across = pl.BlockSpec((step, wide), lambda i: (i, 0))
    return pl.pallas_call(
        kernel,
        grid=(rows // step,),
        in_specs=[pl.BlockSpec((step, depth), lambda i: (i, 0))]
        + weight_specs(pieces, low, wide)
        + [across] * len(received)
        + [pl.BlockSpec((step, width), lambda i: (i, start // width))],
        out_specs=(pl.BlockSpec((step, width), lambda i: (i, 0)), across),
        out_shape=(
            jax.ShapeDtypeStruct((rows, width), jnp.bfloat16),
            jax.ShapeDtypeStruct((rows, wide), jnp.bfloat16),
        ),
        cost_estimate=cost(2 * rows * depth * wide, (lhs, *received)),
        name="gates",
    )(lhs, *pieces, *received, cotangents)


def outer_sums(lhs_parts, grad_parts, first, count, received, first_received, dtype):
    parts = len(lhs_parts)
    rows, wide = grad_parts[0].shape
    step = tile(count)

    def kernel(*refs):
        total = None
        for k in range(parts):
            term = dot(refs[k][...], refs[parts + k][...], 0, 0)
            total = term if total is None else total + term
        for ref in refs[2 * parts : -1]:
            total = total + ref[...].astype(jnp.float32)
        refs[-1][...] = total.astype(dtype)

    out = jax.ShapeDtypeStruct((count, wide), dtype)
    return pl.pallas_call(
        kernel,
        grid=(count // step,),
        in_specs=[pl.BlockSpec((rows, step), lambda i: (0, first // step + i))] * parts
        + [pl.BlockSpec((rows, wide), lambda i: (0, 0))] * parts
        + [pl.BlockSpec((step, wide), lambda i: (first_received // step + i, 0))] * len(received),
        out_specs=pl.BlockSpec((step, wide), lambda i: (i, 0)),
        out_shape=out,
        cost_estimate=cost(2 * rows * parts * count * wide, (*grad_parts, out, out)),
        name="outer_sums",
    )(*lhs_parts, *grad_parts, *received)


def input_sums(grads, weights, first, count, before, dtype):
    parts = len(grads[0])
    pieces = len(weights[0][0])
    depth = weights[0][0][0].shape[0]
    step = tile(count)
    chunks = len(grads)
    across = pl.BlockSpec((parts, step, pieces * depth), lambda i: (0, first // step + i, 0))

    def kernel(*refs):
        grad_refs = refs[: parts * chunks]
        weight_refs = refs[parts * chunks : (parts + pieces) * chunks]
        out_ref = refs[-1]
        for k in range(parts):
            for p in range(pieces):
                columns = slice(p * depth, (p + 1) * depth)
                total = refs[-2][k, :, columns] if before is not None else None
                for c in range(chunks):
                    term = dot(
                        grad_refs[c * parts + k][...], weight_refs[c * pieces + p][...], 1, 1
                    )
                    total = term if total is None else total + term
                out_ref[k, :, columns] = total.astype(dtype)

    out = jax.ShapeDtypeStruct((parts, count, pieces * depth), dtype)
    in_specs, operands = [], []
    for chunk in grads:
        for part in chunk:
            in_specs.append(pl.BlockSpec((step, part.shape[1]), lambda i: (first // step + i, 0)))
            operands.append(part)
    for group, low, wide in weights:
        in_specs += weight_specs(group, low, wide)
        operands += group
    if before is not None:
        in_specs.append(across)
        operands.append(before)
    wide = sum(chunk[0].shape[1] for chunk in grads)
    return pl.pallas_call(
        kernel,
        grid=(count // step,),
        in_specs=in_specs,
        out_specs=pl.BlockSpec((parts, step, pieces * depth), lambda i: (0, i, 0)),
        out_shape=out,
        cost_estimate=cost(2 * parts * count * wide * pieces * depth, (out, out)),
        name="input_sums",
    )(*operands)


def shards(
    bytes_in,
    doc_lengths,
    patch_offsets,
    patch_counts,
    w_query,
    w_key,
    w_value,
    w_proj,
    norm_gain,
    gate_w,
    up_w,
    d_hidden,
):
    bf16, f32 = jnp.bfloat16, jnp.float32
    x_count, core_count = (lax.axis_size(axis) for axis in ROW_AXES)
    a_count, c_count, b_count = (lax.axis_size(axis) for axis in COL_AXES)
    x_own, core_own = (lax.axis_index(axis) for axis in ROW_AXES)
    a_own, c_own, b_own = (lax.axis_index(axis) for axis in COL_AXES)
    states = bytes_in[0]
    length = states.shape[0]
    hop_count = (WINDOW - 2 + length) // length
    first_pos = lax.axis_index(ALL_AXES) * length

    earlier = []
    for distance in range(1, hop_count + 1):
        earlier.insert(0, shifted(states, ALL_AXES, distance))
    queries, key_own, value_own = (
        jnp.dot(states, w, preferred_element_type=f32).astype(bf16) for w in (w_query, w_key, w_value)
    )

    rows, units = gate_w.shape
    sub = units // c_count
    spans = [(start, min(CHUNK, sub - start)) for start in range(0, sub, CHUNK)]
    group_size = (len(spans) + 1) // 2
    groups = [spans[:group_size], spans[group_size:]]
    groups = [(g[0][0], g[-1][0] + g[-1][1], g) for g in groups if g]

    def weight_payload(by, members, gate, up):
        parts = [split(w, c_count, 1) for w in (gate, up)]
        return jnp.concatenate(
            [
                chosen([p[:, first : first + width] for p in side], (c_own + by) % c_count)
                for first, width in members
                for side in parts
            ],
            axis=1,
        )

    def weight_pieces(index, gate, up):
        members = groups[index][2]
        pieces = {}
        for c_by in range(c_count):
            payload = weight_payload(c_by, members, gate, up)
            for b_by in range(b_count):
                if c_by and b_by:
                    pairs = [
                        (c * b_count + b, (c + c_by) % c_count * b_count + (b + b_by) % b_count)
                        for c in range(c_count)
                        for b in range(b_count)
                    ]
                    pieces[b_by, c_by] = lax.ppermute(payload, ("c", "b"), pairs)
                elif c_by:
                    pieces[b_by, c_by] = turned(payload, "c", c_by)
                else:
                    pieces[b_by, c_by] = turned(payload, "b", b_by)
        return [pieces[b_by, c_by] for b_by in range(b_count) for c_by in range(c_count)]

    gate_first, up_first, *earlier = lax.optimization_barrier((gate_w, up_w, *earlier))
    pieces = [weight_pieces(0, gate_first, up_first)]

    late = [
        [jnp.dot(part, w, preferred_element_type=f32).astype(bf16) for w in (w_key, w_value)]
        for part in earlier
    ]
    key_all = jnp.concatenate([pair[0] for pair in late] + [key_own])
    value_all = jnp.concatenate([pair[1] for pair in late] + [value_own])
    query_pos = first_pos + jnp.arange(length, dtype=jnp.int32)
    key_pos = first_pos - hop_count * length + jnp.arange((hop_count + 1) * length, dtype=jnp.int32)
    key_doc = doc_index(doc_lengths, key_pos)
    query_doc = key_doc[hop_count * length :]
    context = byte_layer(
        queries, key_all, value_all, states, query_doc, key_doc, patch_offsets[0], patch_counts[0, 0]
    )
    slot_count = context.shape[0]

    features = jnp.dot(context, w_proj, preferred_element_type=f32).astype(bf16)
    own_float = features.astype(f32)
    model_width = own_float.shape[1]
    own_inverse = lax.rsqrt(jnp.mean(own_float * own_float, axis=1, keepdims=True) + epsilon)
    normed = (own_float * own_inverse * norm_gain).astype(bf16)

    part_width = model_width // a_count
    quarter = part_width // b_count
    a_blocks = split(normed, a_count, 1)

    def columns_for(part, c_by):
        blocks = split(part, c_count * b_count, 1)
        wanted = []
        for b in range(b_count):
            for c in range(c_count):
                place = (c_own + c_by - c) % c_count * b_count + (b_own - b) % b_count
                wanted.append(chosen(blocks, place))
        return jnp.concatenate(wanted, axis=1)

    normed_parts, first_rows = [], []
    for a_by in range(a_count):
        part = turned(chosen(a_blocks, (a_own - a_by) % a_count), "a", -a_by)
        part = jnp.concatenate(
            [turned(columns_for(part, c_by), "c", c_by) for c_by in range(c_count)]
        )
        first_rows.append(part)
        part = jnp.concatenate([turned(part, "x", by) for by in range(x_count)])
        part = jnp.concatenate([turned(part, "core", by) for by in range(core_count)])
        normed_parts.append(part)
    row_count = normed_parts[0].shape[0]

    gate_last, up_last, d_hidden, *_ = lax.optimization_barrier(
        (gate_w, up_w, d_hidden, *first_rows)
    )
    cotangents = split(d_hidden.reshape(-1, units), c_count, 1)
    cotangents = [
        turned(chosen(cotangents, (c_own + c_by) % c_count), "c", c_by)
        for c_by in range(c_count)
    ]

    pieces += [weight_pieces(index, gate_last, up_last) for index in range(1, len(groups))]
    weights = []
    for (start, _, members), group in zip(groups, pieces):
        for first, width in members:
            weights.append((group, 2 * (first - start), 2 * width))

    sums = []
    previous = None
    for weight in weights:
        sent = []
        for a_by in range(1, a_count):
            lhs = normed_parts[a_by] if previous is None else after(normed_parts[a_by], previous)
            previous = partial_sums(lhs, *weight)
            sent.append(turned(previous, "a", a_by))
        sums.append(sent)

    def rows_by_place(array):
        parts = split(array, x_count * core_count, 0)
        return [
            chosen(
                parts, (x_own - x_by) % x_count * core_count + (core_own - core_by) % core_count
            )
            for core_by in range(core_count)
            for x_by in range(x_count)
        ]

    by_place = [rows_by_place(after(part, previous)) for part in cotangents]
    cotangents = jnp.concatenate(
        [by_place[c_by][k] for k in range(x_count * core_count) for c_by in range(c_count)]
    )
    hidden_parts, chunk_grads = [], []
    for index, (start, width) in enumerate(spans):
        lhs = after(normed_parts[0], chunk_grads[-1][0] if index else previous)
        hidden_part, grads = gates(lhs, *weights[index], sums[index], cotangents, start)
        hidden_parts.append(hidden_part)
        chunk_grads.append([turned(grads, "a", -by) for by in range(a_count)])

    weight_grads = []
    input_partial = None
    waiting, done = [], None
    for index, weight in enumerate(weights):
        grads_all = chunk_grads[index]
        if done is not None:
            grads_all = [after(part, done) for part in grads_all]
        received = []
        for by in range(1, b_count):
            partial = outer_sums(normed_parts, grads_all, by * quarter, quarter, [], 0, bf16)
            grads_all = [after(part, partial) for part in grads_all]
            received.append(turned(partial, "b", -by))
        mine = [None] * c_count
        for by in [*range(1, c_count), 0]:
            partial = outer_sums(
                normed_parts, grads_all, by * rows, rows, received, by * rows, bf16 if by else f32
            )
            mine[by] = turned(partial, "c", -by)
        weight_grads.append(mine)
        waiting.append((grads_all, weight))
        if index == len(weights) - 1:
            break
        if index >= len(weights) - 2 or len(waiting) >= 2:
            input_partial = input_sums(
                [pair[0] for pair in waiting],
                [pair[1] for pair in waiting],
                0,
                row_count,
                input_partial,
                f32,
            )
            waiting = []
            done = input_partial

    core_rows = row_count // core_count

    def input_rows(k, dtype):
        return input_sums(
            [pair[0] for pair in waiting],
            [pair[1] for pair in waiting],
            k * core_rows,
            core_rows,
            input_partial,
            dtype,
        )

    sent = [turned(input_rows(k, bf16), "core", -k) for k in range(1, core_count)]
    own_rows = input_rows(0, f32)
    for received in sent:
        own_rows = own_rows + received.astype(f32)
    pieces_by_b = []
    for b_by in range(b_count):
        part = own_rows[:, :, b_by * quarter : (b_by + 1) * quarter]
        part = part.reshape(a_count, x_count, c_count * slot_count, quarter)
        order = lambda sent, k: jnp.concatenate(
            [
                split(sent, c_count, 2)[(c + k) % c_count]
                for c in range(c_count)
            ],
            axis=2,
        )
        if b_by % 2 == 0:
            part = own_sum(part, "x", 1).reshape(a_count, c_count * slot_count, quarter)
            part = own_sum(part, "c", 1, order)
        else:
            part = part.reshape(a_count, x_count, c_count, slot_count, quarter)
            part = part.transpose(0, 2, 1, 3, 4).reshape(
                a_count, c_count * x_count * slot_count, quarter
            )
            part = own_sum(part, "c", 1, order)
            part = own_sum(part, "x", 1)
        pieces_by_b.append(
            [part[0]]
            + [turned(part[by].astype(bf16), "a", by).astype(f32) for by in range(1, a_count)]
        )
    columns = []
    for a in range(a_count):
        ranked = []
        for b_by in range(b_count):
            whole = chosen(
                [pieces_by_b[b_by][(-k) % a_count] for k in range(a_count)], (a - a_own) % a_count
            )
            ranked.append(split(whole, c_count, 1))
        for c in range(c_count):
            for b in range(b_count):
                options = [
                    chosen([ranked[b_by][k] for k in range(c_count)], (c_own - c) % c_count)
                    for b_by in range(b_count)
                ]
                columns.append(chosen(options, (b_own - b) % b_count))
    normed_grad = jnp.concatenate(columns, axis=1)
    scaled = norm_gain * normed_grad
    patch_grad = own_inverse * scaled - own_float * (
        own_inverse * own_inverse * own_inverse
    ) * jnp.mean(scaled * own_float, axis=1, keepdims=True)

    hidden_own = jnp.concatenate(hidden_parts, axis=1).reshape(
        core_count * x_count, c_count, slot_count, sub
    )
    hidden_own = [
        after(turned(hidden_own[:, by].reshape(-1, sub), "c", -by), own_rows)
        for by in range(c_count)
    ]
    hidden_rows = [split(part, core_count * x_count, 0) for part in hidden_own]
    hidden = []
    for x in range(x_count):
        for core in range(core_count):
            place = (core_own - core) % core_count * x_count + (x_own - x) % x_count
            parts = [chosen(part, place) for part in hidden_rows]
            hidden.append(
                jnp.concatenate(
                    [chosen(parts, (k - c_own) % c_count) for k in range(c_count)], axis=1
                )
            )
    hidden = jnp.stack(hidden)

    outs = []
    for side in range(2):
        blocks = [
            jnp.concatenate(
                [
                    mine[by][:, side * width : (side + 1) * width].astype(f32)
                    for (start, width), mine in zip(spans, weight_grads)
                ],
                axis=1,
            )
            for by in range(c_count)
        ]
        outs.append(
            jnp.concatenate(
                [chosen(blocks, (k - c_own) % c_count) for k in range(c_count)], axis=1
            )
        )
    return (hidden, outs[0], outs[1], patch_grad[None])


def halved(count):
    return 2 if count % 2 == 0 else 1


def solution(mesh):
    seq_count, fsdp_count = mesh.shape["seq"], mesh.shape["fsdp"]
    core_count = halved(seq_count)

    def step(*args):
        units = args[9].shape[1] // seq_count
        c_count = 2 if fsdp_count % 2 == 0 and units % 256 == 0 else 1
        b_count = 1
        while fsdp_count // c_count % (4 * b_count * b_count) == 0:
            b_count *= 2
        fine = Mesh(
            mesh.devices.reshape(
                seq_count // core_count,
                core_count,
                fsdp_count // (b_count * c_count),
                c_count,
                b_count,
            ),
            ALL_AXES,
        )
        return jax.shard_map(
            shards,
            mesh=fine,
            in_specs=(
                P(ROW_AXES, COL_AXES, None),
                P(),
                P(ROW_AXES, COL_AXES),
                P(ROW_AXES, COL_AXES),
                P(),
                P(),
                P(),
                P(),
                P(),
                P(COL_AXES, ROW_AXES),
                P(COL_AXES, ROW_AXES),
                P(None, COL_AXES, ROW_AXES),
            ),
            out_specs=(
                P(None, COL_AXES, ROW_AXES),
                P(COL_AXES, ROW_AXES),
                P(COL_AXES, ROW_AXES),
                P(ROW_AXES, COL_AXES, None),
            ),
            check_vma=False,
        )(*args)

    return step
```
